32 devices in a mesh: dp: 4 (over y, x), vocab: 8 (over z, core).
Axes of the slice: x: 2, y: 2, z: 4, core: 2. Of those that a mesh axis runs over, the one named last changes fastest.
Arguments:
- logits: bfloat16 [32, 8, 152064], P('dp', None, 'vocab'), may hold values from -40 to 250
- draft_probs: bfloat16 [32, 8, 152064], P('dp', None, 'vocab'), may hold values from 5.9185606e-07 to 1, as said below
- draft_tokens: int32 [32, 8], P('dp'), may hold values from 0 to 152063
- draft_lengths: int32 [32], P('dp'), may hold values from 1 to 8
- owner_group: int32 [32], P('dp'), may hold values from 0 to 3, as said below
Outputs:
- correction: bfloat16 [64, 152064], P('dp', 'vocab')
- accept_ratio: float32 [64, 8], P('dp')
- expected_accepted: float32 [64], P('dp')
The draws below stay inside these ranges and needn't reach their ends.
Inputs may be any that keep to these rules, and one draw needn't show every extreme that they name: Each row of draft_probs is a distribution over the whole vocabulary whose entries are all positive. `owner_group`: no group hands more than 4 sequences to one group; some group receives exactly 4 sequences from every group.
All inputs are finite; a program needn't handle non-finite values.
Results may differ from the reference program's by a relative error of at most 0.001.
Values may be sent and summed in bfloat16 or wider, within the bound.
A program may use at most 64 MiB of HBM per device.

```python
import math
import jax
import jax.numpy as jnp
from jax import lax

VOCAB = 152064
DRAFT_MAX = 8
SEQ_DEV = 8
CAP = 4
SEQS = 32
SLOTS = 64
N_DP = 4


def logit_field(key):
    root_key = jax.random.fold_in(key, 11)
    key_base = jax.random.fold_in(root_key, 1)
    key_rows = jax.random.fold_in(root_key, 2)
    key_cols = jax.random.fold_in(root_key, 3)
    shape = (SEQS, DRAFT_MAX, VOCAB)
    row_scale = jnp.exp(jax.random.uniform(key_rows, (SEQS, DRAFT_MAX, 1), jnp.float32, math.log(1.5), math.log(4.0)))
    col_scale = jnp.exp(jax.random.uniform(key_cols, (1, 1, VOCAB), jnp.float32, 0.0, math.log(3.2)))
    base = jax.random.normal(key_base, shape, jnp.float32)
    scores = jnp.clip(base * row_scale * col_scale, -40.0, 40.0)
    return scores


def draw_logits(key, part):
    return logit_field(key).astype(jnp.bfloat16)


def draw_draft_probs(key, part):
    scores = logit_field(key)
    noise = 1.5 * jax.random.normal(jax.random.fold_in(key, 23), scores.shape, jnp.float32)
    proposal = jax.nn.softmax(0.7 * scores + noise, axis=2)
    return (0.9 * proposal + 0.1 / VOCAB).astype(jnp.bfloat16)


def draw_owner_group(key, part):
    groups = SEQS // SEQ_DEV
    root_key = jax.random.fold_in(key, 31)
    favoured = jax.random.randint(jax.random.fold_in(root_key, 1), (), 0, groups)
    slot_owner = jnp.arange(groups * CAP, dtype=jnp.int32) // CAP
    block_keys = jax.random.split(jax.random.fold_in(root_key, 2), groups)

    def one_block(block_key):
        key_order = jax.random.fold_in(block_key, 1)
        key_shuffle = jax.random.fold_in(block_key, 2)
        shuffle = jax.random.permutation(key_order, groups * CAP).astype(jnp.int32)
        priority = jnp.where(slot_owner == favoured, -1, shuffle)
        picked = jnp.argsort(priority, stable=True)[:SEQ_DEV]
        owners = slot_owner[picked]
        return owners[jax.random.permutation(key_shuffle, SEQ_DEV)]
    return jax.vmap(one_block)(block_keys).reshape(SEQS).astype(jnp.int32)


def touch_ends(values, key, least, top_value):
    spot = [jax.random.randint(jax.random.fold_in(key, axis), (), 0, length) for axis, length in enumerate(values.shape)]
    widest = values.shape.index(max(values.shape))
    beside = spot[:widest] + [(spot[widest] + 1) % values.shape[widest]] + spot[widest + 1:]
    return values.at[tuple(spot)].set(least).at[tuple(beside)].set(top_value)


def setup_inputs(seed: int = 0) -> dict:
    arg_keys = jax.random.split(jax.random.key(seed), 6)
    return {
        "logits": draw_logits(jax.random.fold_in(arg_keys[5], 71), 0),
        "draft_probs": draw_draft_probs(jax.random.fold_in(arg_keys[5], 71), 0),
        "draft_tokens": touch_ends(jax.random.randint(arg_keys[2], (SEQS, DRAFT_MAX), 0, VOCAB), jax.random.fold_in(arg_keys[2], 1), 0, VOCAB - 1).astype(jnp.int32),
        "draft_lengths": touch_ends(jax.random.randint(arg_keys[3], (SEQS,), 1, DRAFT_MAX + 1), jax.random.fold_in(arg_keys[3], 1), 1, DRAFT_MAX).astype(jnp.int32),
        "owner_group": draw_owner_group(jax.random.fold_in(arg_keys[5], 71), 0),
    }


mixing = 0.1


def verify_group(packed):
    logits, draft_probs, tokens, lengths = packed
    scores = logits.astype(jnp.float32)
    top = jnp.max(scores, axis=2)
    shifted = jnp.exp(scores - top[:, :, None])
    row_total = jnp.sum(shifted, axis=2)
    target = shifted / row_total[:, :, None]
    proposal = draft_probs.astype(jnp.float32)
    index = tokens[:, :, None].astype(jnp.int32)
    picked_target = jnp.take_along_axis(target, index, axis=2)[:, :, 0]
    picked_draft = jnp.take_along_axis(proposal, index, axis=2)[:, :, 0]
    position = lax.broadcasted_iota(jnp.int32, tokens.shape, 1)
    is_live = position < lengths[:, None]
    safe_draft = jnp.where(is_live, picked_draft, 1.0)
    accept = jnp.where(is_live, jnp.minimum(1.0, picked_target / safe_draft), 0.0)
    excess = jnp.maximum(target - proposal, 0.0)
    spread = jnp.sum(excess, axis=2)
    residual = (excess + mixing * target) / (spread + mixing)[:, :, None]
    survive = jnp.cumprod(accept, axis=1)
    before = jnp.concatenate([jnp.ones_like(survive[:, :1]), survive[:, :-1]], axis=1)
    weight = jnp.where(is_live, before * (1.0 - accept), 0.0)
    corrected = jnp.sum(weight[:, :, None] * residual, axis=1).astype(jnp.bfloat16)
    expected = jnp.sum(survive, axis=1)
    return corrected, accept, expected


def reference(logits, draft_probs, draft_tokens, draft_lengths, owner_group):
    grouped = (logits.reshape(N_DP, SEQ_DEV, DRAFT_MAX, VOCAB),
               draft_probs.reshape(N_DP, SEQ_DEV, DRAFT_MAX, VOCAB),
               draft_tokens.reshape(N_DP, SEQ_DEV, DRAFT_MAX),
               draft_lengths.reshape(N_DP, SEQ_DEV))
    corrected, accept, expected = lax.map(verify_group, grouped)
    owners = owner_group.reshape(N_DP, SEQ_DEV).astype(jnp.int32)
    position = jnp.arange(SEQ_DEV, dtype=jnp.int32)
    earlier = position[None, :] < position[:, None]
    same = owners[:, :, None] == owners[:, None, :]
    slot_rank = jnp.sum(jnp.where(same & earlier[None], 1, 0), axis=2).astype(jnp.int32)
    source = jnp.arange(N_DP, dtype=jnp.int32)[:, None]
    landing = (owners * (N_DP * CAP) + source * CAP + slot_rank).reshape(SEQS).astype(jnp.int32)
    correction = jnp.zeros((SLOTS, VOCAB), corrected.dtype).at[landing].set(corrected.reshape(SEQS, VOCAB))
    accept_ratio = jnp.zeros((SLOTS, DRAFT_MAX), accept.dtype).at[landing].set(accept.reshape(SEQS, DRAFT_MAX))
    expected_accepted = jnp.zeros((SLOTS,), expected.dtype).at[landing].set(expected.reshape(SEQS))
    return correction, accept_ratio, expected_accepted
```

```python
import functools

import jax
import jax.numpy as jnp
from jax import lax
from jax.experimental import pallas as pl
from jax.experimental.pallas import tpu as pltpu
from jax.sharding import PartitionSpec as P

mixing = 0.1
LANES = 128
GROUP = 8
CHUNKS = 4
LOW = -1e30
MESH = pl.DeviceIdType.MESH


def sweep(start, stop, fn, carry):
    whole = (stop - start) // GROUP

    def step(i, c):
        base = start + i * GROUP
        return fn(base, GROUP, c)

    if whole:
        carry = lax.fori_loop(0, whole, step, carry)
    rest = (stop - start) % GROUP
    if rest:
        carry = fn(start + whole * GROUP, rest, carry)
    return carry


def lane_tile(i):
    return pl.ds(pl.multiple_of(i * LANES, LANES), LANES)


def kernel(
    dims,
    tok, lens, own, x_hbm, d_hbm,
    out, small_out,
    x, d, e, send, stat_in, spread_in, small,
    load_sem, stat_ssem, stat_rsem, spr_ssem, spr_rsem, out_ssem, out_rsem, sm_ssem, sm_rsem, local_sem,
):
    groups, vocab, capacity = dims
    seqs, depth, width = x_hbm.shape
    full = width // LANES
    tail = width - full * LANES
    tiles = e.shape[0]
    my_dp = lax.axis_index("dp")
    my_v = lax.axis_index("vocab")

    loads = []
    for n in range(seqs):
        loads.append(pltpu.make_async_copy(x_hbm.at[n], x.at[n], load_sem.at[n]))
    for n in range(seqs):
        loads.append(pltpu.make_async_copy(d_hbm.at[n], d.at[n], load_sem.at[seqs + n]))
    for n in range(seqs):
        loads[n].start()
        loads[seqs + n].start()

    barrier = pltpu.get_barrier_semaphore()
    v_peers = [lax.rem(my_v + k, vocab) for k in range(1, vocab)]
    g_peers = [lax.rem(my_dp + k, groups) for k in range(1, groups)]
    for p in v_peers:
        pl.semaphore_signal(barrier, inc=1, device_id=(my_dp, p), device_id_type=MESH)
    for p in g_peers:
        pl.semaphore_signal(barrier, inc=1, device_id=(p, my_v), device_id_type=MESH)

    sub = lax.broadcasted_iota(jnp.int32, (depth, LANES), 0)
    lane = lax.broadcasted_iota(jnp.int32, (depth, LANES), 1)
    zero = jnp.zeros((depth, LANES), jnp.float32)

    def tail_tile(ref, n, fill):
        part = ref[n, :, pl.ds(full * LANES, tail)].astype(jnp.float32)
        return jnp.concatenate([part, jnp.full((depth, LANES - tail), fill, jnp.float32)], axis=1)

    tops = zero
    sums = zero
    column0 = my_v * width
    for n in range(seqs):
        loads[n].wait()
        spot = jnp.zeros((depth, LANES), jnp.int32)
        for j in range(depth):
            spot = jnp.where(sub == j, tok[n, j], spot)
        spot = spot - column0 - lane

        def peak(base, count, c, n=n):
            c = list(c)
            for k in range(count):
                c[k % 4] = jnp.maximum(c[k % 4], x[n, :, lane_tile(base + k)].astype(jnp.float32))
            return tuple(c)

        first = tail_tile(x, n, LOW) if tail else jnp.full((depth, LANES), LOW, jnp.float32)
        c = sweep(0, full, peak, (first,) * 4)
        top = jnp.maximum(jnp.maximum(c[0], c[1]), jnp.maximum(c[2], c[3]))
        top = jnp.broadcast_to(jnp.max(top, axis=1, keepdims=True), (depth, LANES))

        loads[seqs + n].wait()

        def expo(base, count, c, n=n, top=top, spot=spot):
            c = list(c)
            for k in range(count):
                raw = x[n, :, lane_tile(base + k)].astype(jnp.float32)
                value = jnp.exp(raw - top)
                e[base + k, pl.ds(n * depth, depth), :] = value
                c[k % 4] = c[k % 4] + value
                hit = spot == (base + k) * LANES
                c[4] = jnp.where(hit, raw, c[4])
                c[5] = jnp.where(hit, d[n, :, lane_tile(base + k)].astype(jnp.float32), c[5])
            return tuple(c)

        first = zero
        picked_x = zero
        picked_d = zero
        if tail:
            raw = tail_tile(x, n, LOW)
            first = jnp.exp(raw - top)
            e[full, pl.ds(n * depth, depth), :] = first
            hit = (spot == full * LANES) & (lane < tail)
            picked_x = jnp.where(hit, raw, zero)
            picked_d = jnp.where(hit, tail_tile(d, n, 0.0), zero)
        c = sweep(0, full, expo, (first, zero, zero, zero, picked_x, picked_d))
        total = jnp.sum((c[0] + c[1]) + (c[2] + c[3]), axis=1, keepdims=True)
        tops = jnp.where(lax.rem(lane, seqs) == n, top, tops)
        sums = jnp.where(lane == n, total, sums)
        sums = jnp.where(lane == seqs + n, jnp.sum(c[4], axis=1, keepdims=True), sums)
        sums = jnp.where(lane == 2 * seqs + n, jnp.sum(c[5], axis=1, keepdims=True), sums)

    pl.semaphore_wait(barrier, vocab - 1 + groups - 1)

    def exchange(buf, ssem, rsem):
        copies = []
        for k in range(1, vocab):
            to = lax.rem(my_v + k, vocab)
            copies.append(pltpu.make_async_remote_copy(
                src_ref=buf.at[my_v], dst_ref=buf.at[my_v],
                send_sem=ssem.at[k], recv_sem=rsem.at[my_v],
                device_id=(my_dp, to), device_id_type=MESH,
            ))
            copies[-1].start()
        return copies

    def arrive(buf, ssem, rsem):
        for k in range(1, vocab):
            source = lax.rem(my_v + k, vocab)
            pltpu.make_async_remote_copy(
                src_ref=buf.at[source], dst_ref=buf.at[source],
                send_sem=ssem.at[k], recv_sem=rsem.at[source],
                device_id=(my_dp, source), device_id_type=MESH,
            ).wait_recv()

    stat_in[my_v, 0:depth, :] = tops
    stat_in[my_v, depth:2 * depth, :] = sums
    stat_copies = exchange(stat_in, stat_ssem, stat_rsem)

    lens_row = jnp.zeros((depth, LANES), jnp.int32)
    slots = []
    for n in range(seqs):
        lens_row = jnp.where(lane == n, lens[n], lens_row)
        rank = jnp.int32(0)
        for i in range(n):
            rank = rank + jnp.where(own[i] == own[n], 1, 0)
        slots.append(own[n] * capacity + rank)
    live = sub < lens_row
    rows = groups * capacity
    pick_row = lax.broadcasted_iota(jnp.int32, (rows, seqs), 0)
    pick_col = lax.broadcasted_iota(jnp.int32, (rows, seqs), 1)
    picker = jnp.zeros((rows, seqs), jnp.float32)
    for n in range(seqs):
        picker = jnp.where((pick_col == n) & (pick_row == slots[n]), 1.0, picker)
    picker = picker.astype(jnp.bfloat16)

    arrive(stat_in, stat_ssem, stat_rsem)
    peak_all = tops
    for p in range(vocab):
        peak_all = jnp.maximum(peak_all, stat_in[p, 0:depth, :])
    merged = zero
    for p in range(vocab):
        factor = jnp.where(lane < seqs, jnp.exp(stat_in[p, 0:depth, :] - peak_all), 1.0)
        merged = merged + stat_in[p, depth:2 * depth, :] * factor
    scale = jnp.exp(tops - peak_all) / merged

    excess_sum = zero
    for n in range(seqs):
        scale_n = jnp.broadcast_to(scale[:, n:n + 1], (depth, LANES))

        def gap(base, count, c, n=n, scale_n=scale_n):
            c = list(c)
            for k in range(count):
                place = (base + k, pl.ds(n * depth, depth), slice(None))
                target = e[place] * scale_n
                over = jnp.maximum(target - d[n, :, lane_tile(base + k)].astype(jnp.float32), 0.0)
                e[place] = over + mixing * target
                c[k % 4] = c[k % 4] + over
            return tuple(c)

        first = zero
        if tail:
            place = (full, pl.ds(n * depth, depth), slice(None))
            target = e[place] * scale_n
            first = jnp.maximum(target - tail_tile(d, n, 0.0), 0.0)
            e[place] = first + mixing * target
        c = sweep(0, full, gap, (first, zero, zero, zero))
        total = jnp.sum((c[0] + c[1]) + (c[2] + c[3]), axis=1, keepdims=True)
        excess_sum = jnp.where(lane == n, total, excess_sum)

    spread_in[my_v] = excess_sum
    spread_copies = exchange(spread_in, spr_ssem, spr_rsem)

    chosen = pltpu.roll(merged, LANES - seqs, 1)
    drafted = pltpu.roll(merged, LANES - 2 * seqs, 1)
    safe_draft = jnp.where(live, drafted, 1.0)
    accept = jnp.where(live, jnp.minimum(1.0, jnp.exp(chosen - peak_all) / merged / safe_draft), 0.0)
    before = []
    running = jnp.ones((1, LANES), jnp.float32)
    expected = jnp.zeros((1, LANES), jnp.float32)
    for j in range(depth):
        before.append(running)
        running = running * accept[j:j + 1, :]
        expected = expected + running
    before = jnp.concatenate(before, axis=0)
    weight = jnp.where(live, before * (1.0 - accept), 0.0)

    sent_accept = zero
    sent_expected = zero
    expected = jnp.broadcast_to(expected, (depth, LANES))
    for n in range(seqs):
        at_slot = lane == slots[n]
        sent_accept = jnp.where(at_slot, accept[:, n:n + 1], sent_accept)
        sent_expected = jnp.where(at_slot, expected[:, n:n + 1], sent_expected)
    for g in range(groups):
        shift = (LANES - g * capacity) % LANES
        small[g, 0:depth, :] = pltpu.roll(sent_accept, shift, 1) if shift else sent_accept
        small[g, depth:2 * depth, :] = pltpu.roll(sent_expected, shift, 1) if shift else sent_expected
    routed = []
    for k in range(1, groups):
        to = lax.rem(my_dp + k, groups)
        routed.append(pltpu.make_async_remote_copy(
            src_ref=small.at[to], dst_ref=small_out.at[my_dp],
            send_sem=sm_ssem.at[k], recv_sem=sm_rsem.at[my_dp],
            device_id=(to, my_v), device_id_type=MESH,
        ))
        routed[-1].start()
    own_copies = [pltpu.make_async_copy(small.at[my_dp], small_out.at[my_dp], local_sem.at[CHUNKS])]
    own_copies[0].start()

    arrive(spread_in, spr_ssem, spr_rsem)
    spread = spread_in[0]
    for p in range(1, vocab):
        spread = spread + spread_in[p]
    coef = weight / (spread + mixing)
    diag = lax.broadcasted_iota(jnp.int32, (seqs, LANES), 0) == lax.broadcasted_iota(jnp.int32, (seqs, LANES), 1)
    coefs = []
    for j in range(depth):
        row = jnp.where(diag, jnp.broadcast_to(coef[j:j + 1, :], (seqs, LANES)), 0.0)
        coefs.append(jnp.broadcast_to(jnp.sum(row, axis=1, keepdims=True), (seqs, LANES)))

    bounds = [tiles * c // CHUNKS for c in range(CHUNKS + 1)]
    for c in range(CHUNKS):
        def mix(base, count, carry):
            pieces = []
            for k in range(count):
                total = e[base + k, pl.ds(0, seqs, stride=depth), :] * coefs[0]
                for j in range(1, depth):
                    total = total + e[base + k, pl.ds(j, seqs, stride=depth), :] * coefs[j]
                pieces.append(total)
            mixed = pieces[0] if count == 1 else jnp.concatenate(pieces, axis=1)
            sent = jnp.dot(picker, mixed.astype(jnp.bfloat16), preferred_element_type=jnp.float32)
            columns = pl.ds(pl.multiple_of(base * LANES, LANES), count * LANES)
            for g in range(groups):
                send[g, :, columns] = sent[g * capacity:(g + 1) * capacity, :].astype(jnp.bfloat16)
            return carry

        sweep(bounds[c], bounds[c + 1], mix, 0)
        columns = pl.ds(bounds[c] * LANES, (bounds[c + 1] - bounds[c]) * LANES)
        for k in range(1, groups):
            to = lax.rem(my_dp + k, groups)
            routed.append(pltpu.make_async_remote_copy(
                src_ref=send.at[to, :, columns], dst_ref=out.at[my_dp, :, columns],
                send_sem=out_ssem.at[c, k], recv_sem=out_rsem.at[c, my_dp],
                device_id=(to, my_v), device_id_type=MESH,
            ))
            routed[-1].start()
        own_copies.append(pltpu.make_async_copy(
            send.at[my_dp, :, columns], out.at[my_dp, :, columns], local_sem.at[c]))
        own_copies[-1].start()

    for k in range(1, groups):
        source = lax.rem(my_dp + k, groups)
        pltpu.make_async_remote_copy(
            src_ref=small.at[source], dst_ref=small_out.at[source],
            send_sem=sm_ssem.at[k], recv_sem=sm_rsem.at[source],
            device_id=(source, my_v), device_id_type=MESH,
        ).wait_recv()
    for c in range(CHUNKS):
        columns = pl.ds(bounds[c] * LANES, (bounds[c + 1] - bounds[c]) * LANES)
        for k in range(1, groups):
            source = lax.rem(my_dp + k, groups)
            pltpu.make_async_remote_copy(
                src_ref=send.at[source, :, columns], dst_ref=out.at[source, :, columns],
                send_sem=out_ssem.at[c, k], recv_sem=out_rsem.at[c, source],
                device_id=(source, my_v), device_id_type=MESH,
            ).wait_recv()
    for copy in own_copies:
        copy.wait()
    for copy in stat_copies + spread_copies + routed:
        copy.wait_send()


def body(logits, draft_probs, draft_tokens, draft_lengths, owner_group):
    groups = lax.axis_size("dp")
    vocab = lax.axis_size("vocab")
    seqs, depth, width = logits.shape
    capacity = max(2, 2 * seqs // groups)
    tiles = -(-width // LANES)
    padded = tiles * LANES
    smem = pl.BlockSpec(memory_space=pltpu.SMEM)
    hbm = pl.BlockSpec(memory_space=pl.ANY)
    dma = pltpu.SemaphoreType.DMA
    out, small = pl.pallas_call(
        functools.partial(kernel, (groups, vocab, capacity)),
        out_shape=(
            jax.ShapeDtypeStruct((groups, capacity, padded), jnp.bfloat16),
            jax.ShapeDtypeStruct((groups, 2 * depth, LANES), jnp.float32),
        ),
        in_specs=[smem, smem, smem, hbm, hbm],
        out_specs=(hbm, hbm),
        scratch_shapes=[
            pltpu.VMEM((seqs, depth, width), jnp.bfloat16),
            pltpu.VMEM((seqs, depth, width), jnp.bfloat16),
            pltpu.VMEM((tiles, seqs * depth, LANES), jnp.float32),
            pltpu.VMEM((groups, capacity, padded), jnp.bfloat16),
            pltpu.VMEM((vocab, 2 * depth, LANES), jnp.float32),
            pltpu.VMEM((vocab, depth, LANES), jnp.float32),
            pltpu.VMEM((groups, 2 * depth, LANES), jnp.float32),
            dma((2 * seqs,)),
            dma((vocab,)),
            dma((vocab,)),
            dma((vocab,)),
            dma((vocab,)),
            dma((CHUNKS, groups)),
            dma((CHUNKS, groups)),
            dma((groups,)),
            dma((groups,)),
            dma((CHUNKS + 1,)),
        ],
        compiler_params=pltpu.CompilerParams(collective_id=0, has_side_effects=True),
    )(draft_tokens, draft_lengths, owner_group, logits, draft_probs)
    correction = out[:, :, :width].reshape(groups * capacity, width)
    accept_ratio = small[:, :depth, :capacity].transpose(0, 2, 1).reshape(groups * capacity, depth)
    expected_accepted = small[:, depth, :capacity].reshape(groups * capacity)
    return (correction, accept_ratio, expected_accepted)


def solution(mesh):
    placed = (P("dp", None, "vocab"), P("dp", None, "vocab"), P("dp", None), P("dp"), P("dp"))
    return jax.shard_map(
        body,
        mesh=mesh,
        in_specs=placed,
        out_specs=(P("dp", "vocab"), P("dp", None), P("dp")),
        check_vma=False,
    )
```

```python
import functools

import jax
import jax.numpy as jnp
from jax import lax
from jax.experimental import pallas as pl
from jax.experimental.pallas import tpu as pltpu
from jax.sharding import PartitionSpec as P

mixing = 0.1
LANES = 128
GROUP = 40
MIX_GROUP = 8
CHUNKS = 5
LOW = -1e30
MESH = pl.DeviceIdType.MESH


def sweep(start, stop, fn, carry, most=GROUP):
    extent = stop - start
    size = max(1, min(most, extent))
    size = min(range(max(1, size // 2), size + 1), key=lambda g: (extent % g, -g))
    whole = extent // size

    def step(i, c):
        return fn(start + i * size, size, c)

    if whole:
        carry = lax.fori_loop(0, whole, step, carry)
    rest = extent % size
    if rest:
        carry = fn(start + whole * size, rest, carry)
    return carry


def lane_tile(i):
    return pl.ds(pl.multiple_of(i * LANES, LANES), LANES)


def kernel(
    dims,
    tok, lens, own, x_hbm, d_hbm,
    out, accept_out, expected_out,
    x, d, e, send, landed, block, stat_in, spread_in, small, small_in,
    load_sem, stat_ssem, stat_rsem, spr_ssem, spr_rsem, out_ssem, out_rsem, sm_ssem, sm_rsem, local_sem, store_sem,
):
    groups, vocab, capacity = dims
    seqs, depth, width = x_hbm.shape
    full = width // LANES
    tail = width - full * LANES
    tiles = e.shape[0]
    my_dp = lax.axis_index("dp")
    my_v = lax.axis_index("vocab")

    loads = []
    for n in range(seqs):
        loads.append(pltpu.make_async_copy(x_hbm.at[n], x.at[n], load_sem.at[n]))
    for n in range(seqs):
        loads.append(pltpu.make_async_copy(d_hbm.at[n], d.at[n], load_sem.at[seqs + n]))
    for n in range(seqs):
        loads[n].start()
        loads[seqs + n].start()

    barrier = pltpu.get_barrier_semaphore()
    v_peers = [lax.rem(my_v + k, vocab) for k in range(1, vocab)]
    g_peers = [lax.rem(my_dp + k, groups) for k in range(1, groups)]
    for p in v_peers:
        pl.semaphore_signal(barrier, inc=1, device_id=(my_dp, p), device_id_type=MESH)
    for p in g_peers:
        pl.semaphore_signal(barrier, inc=1, device_id=(p, my_v), device_id_type=MESH)

    sub = lax.broadcasted_iota(jnp.int32, (depth, LANES), 0)
    lane = lax.broadcasted_iota(jnp.int32, (depth, LANES), 1)
    zero = jnp.zeros((depth, LANES), jnp.float32)

    def tail_tile(ref, n, fill):
        part = ref[n, :, pl.ds(full * LANES, tail)].astype(jnp.float32)
        return jnp.concatenate([part, jnp.full((depth, LANES - tail), fill, jnp.float32)], axis=1)

    tops = zero
    sums = zero
    for n in range(seqs):
        loads[n].wait()

        def peak(base, count, c, n=n):
            c = list(c)
            for k in range(count):
                c[k % 4] = jnp.maximum(c[k % 4], x[n, :, lane_tile(base + k)].astype(jnp.float32))
            return tuple(c)

        first = tail_tile(x, n, LOW) if tail else jnp.full((depth, LANES), LOW, jnp.float32)
        c = sweep(0, full, peak, (first,) * 4)
        top = jnp.maximum(jnp.maximum(c[0], c[1]), jnp.maximum(c[2], c[3]))
        top = jnp.broadcast_to(jnp.max(top, axis=1, keepdims=True), (depth, LANES))

        def expo(base, count, c, n=n, top=top):
            c = list(c)
            for k in range(count):
                raw = x[n, :, lane_tile(base + k)].astype(jnp.float32)
                value = jnp.exp(raw - top)
                e[base + k, pl.ds(n * depth, depth), :] = value
                c[k % 4] = c[k % 4] + value
            return tuple(c)

        first = zero
        if tail:
            raw = tail_tile(x, n, LOW)
            first = jnp.exp(raw - top)
            e[full, pl.ds(n * depth, depth), :] = first
        c = sweep(0, full, expo, (first, zero, zero, zero))
        total = jnp.sum((c[0] + c[1]) + (c[2] + c[3]), axis=1, keepdims=True)
        tops = jnp.where(lane == n, top, tops)
        sums = jnp.where(lane == n, total, sums)
        sums = jnp.where(lane == seqs + n, top, sums)

    pl.semaphore_wait(barrier, vocab - 1 + groups - 1)

    def exchange(buf, ssem, rsem):
        copies = []
        for k in range(1, vocab):
            to = lax.rem(my_v + k, vocab)
            copies.append(pltpu.make_async_remote_copy(
                src_ref=buf.at[my_v], dst_ref=buf.at[my_v],
                send_sem=ssem.at[k], recv_sem=rsem.at[my_v],
                device_id=(my_dp, to), device_id_type=MESH,
            ))
            copies[-1].start()
        return copies

    def arrive(buf, ssem, rsem):
        for k in range(1, vocab):
            source = lax.rem(my_v + k, vocab)
            pltpu.make_async_remote_copy(
                src_ref=buf.at[source], dst_ref=buf.at[source],
                send_sem=ssem.at[k], recv_sem=rsem.at[source],
                device_id=(my_dp, source), device_id_type=MESH,
            ).wait_recv()

    stat_in[my_v] = sums
    stat_copies = exchange(stat_in, stat_ssem, stat_rsem)

    lens_row = jnp.zeros((depth, LANES), jnp.int32)
    slots = []
    for n in range(seqs):
        lens_row = jnp.where(lane == n, lens[n], lens_row)
        rank = jnp.int32(0)
        for i in range(n):
            rank = rank + jnp.where(own[i] == own[n], 1, 0)
        slots.append(own[n] * capacity + rank)
    live = sub < lens_row
    rows = groups * capacity
    pick_row = lax.broadcasted_iota(jnp.int32, (rows, seqs), 0)
    pick_col = lax.broadcasted_iota(jnp.int32, (rows, seqs), 1)
    picker = jnp.zeros((rows, seqs), jnp.float32)
    for n in range(seqs):
        picker = jnp.where((pick_col == n) & (pick_row == slots[n]), 1.0, picker)
    picker = picker.astype(jnp.bfloat16)

    column0 = my_v * width
    excess_sum = zero
    for n in range(seqs):
        loads[seqs + n].wait()
        spot = jnp.zeros((depth, LANES), jnp.int32)
        for j in range(depth):
            spot = jnp.where(sub == j, tok[n, j], spot)
        spot = spot - column0 - lane

        def pick(base, count, c, n=n, spot=spot):
            c = list(c)
            for k in range(count):
                hit = spot == (base + k) * LANES
                c[0] = jnp.where(hit, x[n, :, lane_tile(base + k)].astype(jnp.float32), c[0])
                c[1] = jnp.where(hit, d[n, :, lane_tile(base + k)].astype(jnp.float32), c[1])
            return tuple(c)

        first = (zero, zero)
        if tail:
            hit = (spot == full * LANES) & (lane < tail)
            first = (jnp.where(hit, tail_tile(x, n, 0.0), zero), jnp.where(hit, tail_tile(d, n, 0.0), zero))
        c = sweep(0, full, pick, first)
        excess_sum = jnp.where(lane == seqs + n, jnp.sum(c[0], axis=1, keepdims=True), excess_sum)
        excess_sum = jnp.where(lane == 2 * seqs + n, jnp.sum(c[1], axis=1, keepdims=True), excess_sum)

    arrive(stat_in, stat_ssem, stat_rsem)
    parts = [stat_in[p] for p in range(vocab)]
    peaks = [pltpu.roll(part, LANES - seqs, 1) for part in parts]
    peak_all = functools.reduce(jnp.maximum, peaks)
    merged = zero
    for part, local_peak in zip(parts, peaks):
        merged = merged + part * jnp.exp(local_peak - peak_all)
    scale = jnp.exp(tops - peak_all) / merged

    for n in range(seqs):
        scale_n = jnp.broadcast_to(scale[:, n:n + 1], (depth, LANES))

        def gap(base, count, c, n=n, scale_n=scale_n):
            c = list(c)
            for k in range(count):
                place = (base + k, pl.ds(n * depth, depth), slice(None))
                target = e[place] * scale_n
                over = jnp.maximum(target - d[n, :, lane_tile(base + k)].astype(jnp.float32), 0.0)
                e[place] = over + mixing * target
                c[k % 4] = c[k % 4] + over
            return tuple(c)

        first = zero
        if tail:
            place = (full, pl.ds(n * depth, depth), slice(None))
            target = e[place] * scale_n
            first = jnp.maximum(target - tail_tile(d, n, 0.0), 0.0)
            e[place] = first + mixing * target
        c = sweep(0, full, gap, (first, zero, zero, zero))
        total = jnp.sum((c[0] + c[1]) + (c[2] + c[3]), axis=1, keepdims=True)
        excess_sum = jnp.where(lane == n, total, excess_sum)

    spread_in[my_v] = excess_sum
    spread_copies = exchange(spread_in, spr_ssem, spr_rsem)

    arrive(spread_in, spr_ssem, spr_rsem)
    spread = spread_in[0]
    for p in range(1, vocab):
        spread = spread + spread_in[p]
    chosen = pltpu.roll(spread, LANES - seqs, 1)
    drafted = pltpu.roll(spread, LANES - 2 * seqs, 1)
    safe_draft = jnp.where(live, drafted, 1.0)
    accept = jnp.where(live, jnp.minimum(1.0, jnp.exp(chosen - peak_all) / merged / safe_draft), 0.0)
    before = []
    running = jnp.ones((1, LANES), jnp.float32)
    expected = jnp.zeros((1, LANES), jnp.float32)
    for j in range(depth):
        before.append(running)
        running = running * accept[j:j + 1, :]
        expected = expected + running
    before = jnp.concatenate(before, axis=0)
    weight = jnp.where(live, before * (1.0 - accept), 0.0)

    coef = weight / (spread + mixing)
    diag = lax.broadcasted_iota(jnp.int32, (seqs, LANES), 0) == lax.broadcasted_iota(jnp.int32, (seqs, LANES), 1)
    coefs = []
    for j in range(depth):
        row = jnp.where(diag, jnp.broadcast_to(coef[j:j + 1, :], (seqs, LANES)), 0.0)
        coefs.append(jnp.broadcast_to(jnp.sum(row, axis=1, keepdims=True), (seqs, LANES)))

    routed = []
    own_copies = []
    bounds = [tiles * c // CHUNKS for c in range(CHUNKS + 1)]
    for c in range(CHUNKS):
        def mix(base, count, carry):
            pieces = []
            for k in range(count):
                total = e[base + k, pl.ds(0, seqs, stride=depth), :] * coefs[0]
                for j in range(1, depth):
                    total = total + e[base + k, pl.ds(j, seqs, stride=depth), :] * coefs[j]
                pieces.append(total)
            mixed = pieces[0] if count == 1 else jnp.concatenate(pieces, axis=1)
            sent = jnp.dot(picker, mixed.astype(jnp.bfloat16), preferred_element_type=jnp.float32)
            columns = pl.ds(pl.multiple_of(base * LANES, LANES), count * LANES)
            for g in range(groups):
                send[g, :, columns] = sent[g * capacity:(g + 1) * capacity, :].astype(jnp.bfloat16)
            return carry

        sweep(bounds[c], bounds[c + 1], mix, 0, MIX_GROUP)
        columns = pl.ds(bounds[c] * LANES, (bounds[c + 1] - bounds[c]) * LANES)
        for k in range(1, groups):
            to = lax.rem(my_dp + k, groups)
            routed.append(pltpu.make_async_remote_copy(
                src_ref=send.at[to, :, columns], dst_ref=landed.at[my_dp, :, columns],
                send_sem=out_ssem.at[c, k], recv_sem=out_rsem.at[c, my_dp],
                device_id=(to, my_v), device_id_type=MESH,
            ))
            routed[-1].start()
        own_copies.append(pltpu.make_async_copy(
            send.at[my_dp, :, columns], landed.at[my_dp, :, columns], local_sem.at[c]))
        own_copies[-1].start()

    sent_accept = zero
    sent_expected = zero
    expected = jnp.broadcast_to(expected, (depth, LANES))
    for n in range(seqs):
        at_slot = lane == slots[n]
        sent_accept = jnp.where(at_slot, accept[:, n:n + 1], sent_accept)
        sent_expected = jnp.where(at_slot, expected[:, n:n + 1], sent_expected)
    for g in range(groups):
        shift = (LANES - g * capacity) % LANES
        small[g, 0:depth, :] = pltpu.roll(sent_accept, shift, 1) if shift else sent_accept
        small[g, depth:2 * depth, :] = pltpu.roll(sent_expected, shift, 1) if shift else sent_expected
    for k in range(1, groups):
        to = lax.rem(my_dp + k, groups)
        routed.append(pltpu.make_async_remote_copy(
            src_ref=small.at[to], dst_ref=small_in.at[my_dp],
            send_sem=sm_ssem.at[k], recv_sem=sm_rsem.at[my_dp],
            device_id=(to, my_v), device_id_type=MESH,
        ))
        routed[-1].start()
    stores = []
    for c in range(CHUNKS):
        columns = pl.ds(bounds[c] * LANES, (bounds[c + 1] - bounds[c]) * LANES)
        for k in range(1, groups):
            source = lax.rem(my_dp + k, groups)
            pltpu.make_async_remote_copy(
                src_ref=send.at[source, :, columns], dst_ref=landed.at[source, :, columns],
                send_sem=out_ssem.at[c, k], recv_sem=out_rsem.at[c, source],
                device_id=(source, my_v), device_id_type=MESH,
            ).wait_recv()
        own_copies[c].wait()

        def gather(base, count, carry):
            span = pl.ds(pl.multiple_of(base * LANES, LANES), count * LANES)
            pieces = [landed[g, :, span].astype(jnp.float32) for g in range(groups)]
            block[:, span] = jnp.concatenate(pieces, axis=0).astype(jnp.bfloat16)
            return carry

        sweep(bounds[c], bounds[c + 1], gather, 0, MIX_GROUP)
        stores.append(pltpu.make_async_copy(block.at[:, columns], out.at[:, columns], store_sem.at[c]))
        stores[-1].start()
    small_in[my_dp] = small[my_dp]
    for k in range(1, groups):
        source = lax.rem(my_dp + k, groups)
        pltpu.make_async_remote_copy(
            src_ref=small.at[source], dst_ref=small_in.at[source],
            send_sem=sm_ssem.at[k], recv_sem=sm_rsem.at[source],
            device_id=(source, my_v), device_id_type=MESH,
        ).wait_recv()
    final_accept = zero
    final_expected = zero
    for g in range(groups):
        mine = (lane >= g * capacity) & (lane < (g + 1) * capacity)
        final_accept = jnp.where(mine, pltpu.roll(small_in[g, 0:depth, :], g * capacity, 1), final_accept)
        final_expected = jnp.where(mine, pltpu.roll(small_in[g, depth:2 * depth, :], g * capacity, 1), final_expected)
    accept_out[...] = final_accept[:, :rows]
    expected_out[...] = final_expected[0:1, :rows]
    for copy in stores:
        copy.wait()
    for copy in stat_copies + spread_copies + routed:
        copy.wait_send()


def body(logits, draft_probs, draft_tokens, draft_lengths, owner_group):
    groups = lax.axis_size("dp")
    vocab = lax.axis_size("vocab")
    seqs, depth, width = logits.shape
    capacity = max(2, 2 * seqs // groups)
    tiles = -(-width // LANES)
    padded = tiles * LANES
    smem = pl.BlockSpec(memory_space=pltpu.SMEM)
    hbm = pl.BlockSpec(memory_space=pl.ANY)
    dma = pltpu.SemaphoreType.DMA
    slots = groups * capacity
    vmem = pl.BlockSpec(memory_space=pltpu.VMEM)
    out, accept, expected = pl.pallas_call(
        functools.partial(kernel, (groups, vocab, capacity)),
        out_shape=(
            jax.ShapeDtypeStruct((slots, padded), jnp.bfloat16),
            jax.ShapeDtypeStruct((depth, slots), jnp.float32),
            jax.ShapeDtypeStruct((1, slots), jnp.float32),
        ),
        in_specs=[smem, smem, smem, hbm, hbm],
        out_specs=(hbm, vmem, vmem),
        scratch_shapes=[
            pltpu.VMEM((seqs, depth, width), jnp.bfloat16),
            pltpu.VMEM((seqs, depth, width), jnp.bfloat16),
            pltpu.VMEM((tiles, seqs * depth, LANES), jnp.float32),
            pltpu.VMEM((groups, capacity, padded), jnp.bfloat16),
            pltpu.VMEM((groups, capacity, padded), jnp.bfloat16),
            pltpu.VMEM((slots, padded), jnp.bfloat16),
            pltpu.VMEM((vocab, depth, LANES), jnp.float32),
            pltpu.VMEM((vocab, depth, LANES), jnp.float32),
            pltpu.VMEM((groups, 2 * depth, LANES), jnp.float32),
            pltpu.VMEM((groups, 2 * depth, LANES), jnp.float32),
            dma((2 * seqs,)),
            dma((vocab,)),
            dma((vocab,)),
            dma((vocab,)),
            dma((vocab,)),
            dma((CHUNKS, groups)),
            dma((CHUNKS, groups)),
            dma((groups,)),
            dma((groups,)),
            dma((CHUNKS,)),
            dma((CHUNKS,)),
        ],
        compiler_params=pltpu.CompilerParams(collective_id=0, has_side_effects=True),
    )(draft_tokens, draft_lengths, owner_group, logits, draft_probs)
    correction = out[:, :width]
    accept_ratio = accept.T
    expected_accepted = expected.reshape(slots)
    return (correction, accept_ratio, expected_accepted)


def solution(mesh):
    placed = (P("dp", None, "vocab"), P("dp", None, "vocab"), P("dp", None), P("dp"), P("dp"))
    return jax.shard_map(
        body,
        mesh=mesh,
        in_specs=placed,
        out_specs=(P("dp", "vocab"), P("dp", None), P("dp")),
        check_vma=False,
    )
```

```python
import functools

import jax
import jax.numpy as jnp
from jax import lax
from jax.experimental import pallas as pl
from jax.experimental.pallas import tpu as pltpu
from jax.sharding import PartitionSpec as P

mixing = 0.1
LANES = 128
GROUP = 40
MIX_GROUP = 8
CHUNKS = 5
LOW = -1e30
MESH = pl.DeviceIdType.MESH


def sweep(start, stop, fn, carry, most=GROUP):
    extent = stop - start
    size = max(1, min(most, extent))
    size = min(range(max(1, size // 2), size + 1), key=lambda g: (extent % g, -g))
    whole = extent // size

    def step(i, c):
        return fn(start + i * size, size, c)

    if whole:
        carry = lax.fori_loop(0, whole, step, carry)
    rest = extent % size
    if rest:
        carry = fn(start + whole * size, rest, carry)
    return carry


def lane_tile(i):
    return pl.ds(pl.multiple_of(i * LANES, LANES), LANES)


def kernel(
    dims,
    tok_hbm, lens_hbm, own_hbm, x_hbm, d_hbm,
    out, accept_out, expected_out,
    tok, lens, own, x, d, e, send, landed, block, stat_in, spread_in, small, small_in,
    scalar_sem, load_sem, stat_ssem, stat_rsem, spr_ssem, spr_rsem, out_ssem, out_rsem, sm_ssem, sm_rsem, local_sem, store_sem,
):
    groups, vocab, capacity = dims
    seqs, depth, width = x_hbm.shape
    full = width // LANES
    tail = width - full * LANES
    tiles = e.shape[0]
    my_dp = lax.axis_index("dp")
    my_v = lax.axis_index("vocab")

    loads = []
    for n in range(seqs):
        loads.append(pltpu.make_async_copy(x_hbm.at[n], x.at[n], load_sem.at[n]))
    for n in range(seqs):
        loads.append(pltpu.make_async_copy(d_hbm.at[n], d.at[n], load_sem.at[seqs + n]))
    for n in range(seqs):
        loads[n].start()
    scalars = []
    for i, (source, target) in enumerate(((tok_hbm, tok), (lens_hbm, lens), (own_hbm, own))):
        scalars.append(pltpu.make_async_copy(source, target, scalar_sem.at[i]))
        scalars[-1].start()

    barrier = pltpu.get_barrier_semaphore()
    v_peers = [lax.rem(my_v + k, vocab) for k in range(1, vocab)]
    g_peers = [lax.rem(my_dp + k, groups) for k in range(1, groups)]
    for p in v_peers:
        pl.semaphore_signal(barrier, inc=1, device_id=(my_dp, p), device_id_type=MESH)
    for p in g_peers:
        pl.semaphore_signal(barrier, inc=1, device_id=(p, my_v), device_id_type=MESH)

    sub = lax.broadcasted_iota(jnp.int32, (depth, LANES), 0)
    lane = lax.broadcasted_iota(jnp.int32, (depth, LANES), 1)
    zero = jnp.zeros((depth, LANES), jnp.float32)

    def tail_tile(ref, n, fill):
        part = ref[n, :, pl.ds(full * LANES, tail)].astype(jnp.float32)
        return jnp.concatenate([part, jnp.full((depth, LANES - tail), fill, jnp.float32)], axis=1)

    tops = zero
    sums = zero
    for n in range(seqs):
        loads[n].wait()
        loads[seqs + n].start()

        def peak(base, count, c, n=n):
            c = list(c)
            for k in range(count):
                c[k % 4] = jnp.maximum(c[k % 4], x[n, :, lane_tile(base + k)].astype(jnp.float32))
            return tuple(c)

        first = tail_tile(x, n, LOW) if tail else jnp.full((depth, LANES), LOW, jnp.float32)
        c = sweep(0, full, peak, (first,) * 4)
        top = jnp.maximum(jnp.maximum(c[0], c[1]), jnp.maximum(c[2], c[3]))
        top = jnp.broadcast_to(jnp.max(top, axis=1, keepdims=True), (depth, LANES))

        def expo(base, count, c, n=n, top=top):
            c = list(c)
            for k in range(count):
                raw = x[n, :, lane_tile(base + k)].astype(jnp.float32)
                value = jnp.exp(raw - top)
                e[base + k, pl.ds(n * depth, depth), :] = value
                c[k % 4] = c[k % 4] + value
            return tuple(c)

        first = zero
        if tail:
            raw = tail_tile(x, n, LOW)
            first = jnp.exp(raw - top)
            e[full, pl.ds(n * depth, depth), :] = first
        c = sweep(0, full, expo, (first, zero, zero, zero))
        total = jnp.sum((c[0] + c[1]) + (c[2] + c[3]), axis=1, keepdims=True)
        tops = jnp.where(lane == n, top, tops)
        sums = jnp.where(lane == n, total, sums)
        sums = jnp.where(lane == seqs + n, top, sums)

    pl.semaphore_wait(barrier, vocab - 1 + groups - 1)

    def exchange(buf, ssem, rsem):
        copies = []
        for k in range(1, vocab):
            to = lax.rem(my_v + k, vocab)
            copies.append(pltpu.make_async_remote_copy(
                src_ref=buf.at[my_v], dst_ref=buf.at[my_v],
                send_sem=ssem.at[k], recv_sem=rsem.at[my_v],
                device_id=(my_dp, to), device_id_type=MESH,
            ))
            copies[-1].start()
        return copies

    def arrive(buf, ssem, rsem):
        for k in range(1, vocab):
            source = lax.rem(my_v + k, vocab)
            pltpu.make_async_remote_copy(
                src_ref=buf.at[source], dst_ref=buf.at[source],
                send_sem=ssem.at[k], recv_sem=rsem.at[source],
                device_id=(my_dp, source), device_id_type=MESH,
            ).wait_recv()

    stat_in[my_v] = sums
    stat_copies = exchange(stat_in, stat_ssem, stat_rsem)

    for copy in scalars:
        copy.wait()

    lens_row = jnp.zeros((depth, LANES), jnp.int32)
    slots = []
    for n in range(seqs):
        lens_row = jnp.where(lane == n, lens[n], lens_row)
        rank = jnp.int32(0)
        for i in range(n):
            rank = rank + jnp.where(own[i] == own[n], 1, 0)
        slots.append(own[n] * capacity + rank)
    live = sub < lens_row
    rows = groups * capacity
    pick_row = lax.broadcasted_iota(jnp.int32, (rows, seqs), 0)
    pick_col = lax.broadcasted_iota(jnp.int32, (rows, seqs), 1)
    picker = jnp.zeros((rows, seqs), jnp.float32)
    for n in range(seqs):
        picker = jnp.where((pick_col == n) & (pick_row == slots[n]), 1.0, picker)
    picker = picker.astype(jnp.bfloat16)

    column0 = my_v * width
    excess_sum = zero
    for n in range(seqs):
        loads[seqs + n].wait()
        spot = jnp.zeros((depth, LANES), jnp.int32)
        for j in range(depth):
            spot = jnp.where(sub == j, tok[n, j], spot)
        spot = spot - column0 - lane

        def pick(base, count, c, n=n, spot=spot):
            c = list(c)
            for k in range(count):
                hit = spot == (base + k) * LANES
                c[0] = jnp.where(hit, x[n, :, lane_tile(base + k)].astype(jnp.float32), c[0])
                c[1] = jnp.where(hit, d[n, :, lane_tile(base + k)].astype(jnp.float32), c[1])
            return tuple(c)

        first = (zero, zero)
        if tail:
            hit = (spot == full * LANES) & (lane < tail)
            first = (jnp.where(hit, tail_tile(x, n, 0.0), zero), jnp.where(hit, tail_tile(d, n, 0.0), zero))
        c = sweep(0, full, pick, first)
        excess_sum = jnp.where(lane == seqs + n, jnp.sum(c[0], axis=1, keepdims=True), excess_sum)
        excess_sum = jnp.where(lane == 2 * seqs + n, jnp.sum(c[1], axis=1, keepdims=True), excess_sum)

    arrive(stat_in, stat_ssem, stat_rsem)
    parts = [stat_in[p] for p in range(vocab)]
    peaks = [pltpu.roll(part, LANES - seqs, 1) for part in parts]
    peak_all = functools.reduce(jnp.maximum, peaks)
    merged = zero
    for part, local_peak in zip(parts, peaks):
        merged = merged + part * jnp.exp(local_peak - peak_all)
    scale = jnp.exp(tops - peak_all) / merged

    for n in range(seqs):
        scale_n = jnp.broadcast_to(scale[:, n:n + 1], (depth, LANES))

        def gap(base, count, c, n=n, scale_n=scale_n):
            c = list(c)
            for k in range(count):
                place = (base + k, pl.ds(n * depth, depth), slice(None))
                target = e[place] * scale_n
                over = jnp.maximum(target - d[n, :, lane_tile(base + k)].astype(jnp.float32), 0.0)
                e[place] = over + mixing * target
                c[k % 4] = c[k % 4] + over
            return tuple(c)

        first = zero
        if tail:
            place = (full, pl.ds(n * depth, depth), slice(None))
            target = e[place] * scale_n
            first = jnp.maximum(target - tail_tile(d, n, 0.0), 0.0)
            e[place] = first + mixing * target
        c = sweep(0, full, gap, (first, zero, zero, zero))
        total = jnp.sum((c[0] + c[1]) + (c[2] + c[3]), axis=1, keepdims=True)
        excess_sum = jnp.where(lane == n, total, excess_sum)

    spread_in[my_v] = excess_sum
    spread_copies = exchange(spread_in, spr_ssem, spr_rsem)

    arrive(spread_in, spr_ssem, spr_rsem)
    spread = spread_in[0]
    for p in range(1, vocab):
        spread = spread + spread_in[p]
    chosen = pltpu.roll(spread, LANES - seqs, 1)
    drafted = pltpu.roll(spread, LANES - 2 * seqs, 1)
    safe_draft = jnp.where(live, drafted, 1.0)
    accept = jnp.where(live, jnp.minimum(1.0, jnp.exp(chosen - peak_all) / merged / safe_draft), 0.0)
    before = []
    running = jnp.ones((1, LANES), jnp.float32)
    expected = jnp.zeros((1, LANES), jnp.float32)
    for j in range(depth):
        before.append(running)
        running = running * accept[j:j + 1, :]
        expected = expected + running
    before = jnp.concatenate(before, axis=0)
    weight = jnp.where(live, before * (1.0 - accept), 0.0)

    coef = weight / (spread + mixing)
    diag = lax.broadcasted_iota(jnp.int32, (seqs, LANES), 0) == lax.broadcasted_iota(jnp.int32, (seqs, LANES), 1)
    coefs = []
    for j in range(depth):
        row = jnp.where(diag, jnp.broadcast_to(coef[j:j + 1, :], (seqs, LANES)), 0.0)
        coefs.append(jnp.broadcast_to(jnp.sum(row, axis=1, keepdims=True), (seqs, LANES)))

    routed = []
    own_copies = []
    bounds = [tiles * c // CHUNKS for c in range(CHUNKS + 1)]
    for c in range(CHUNKS):
        def mix(base, count, carry):
            pieces = []
            for k in range(count):
                total = e[base + k, pl.ds(0, seqs, stride=depth), :] * coefs[0]
                for j in range(1, depth):
                    total = total + e[base + k, pl.ds(j, seqs, stride=depth), :] * coefs[j]
                pieces.append(total)
            mixed = pieces[0] if count == 1 else jnp.concatenate(pieces, axis=1)
            sent = jnp.dot(picker, mixed.astype(jnp.bfloat16), preferred_element_type=jnp.float32)
            columns = pl.ds(pl.multiple_of(base * LANES, LANES), count * LANES)
            for g in range(groups):
                send[g, :, columns] = sent[g * capacity:(g + 1) * capacity, :].astype(jnp.bfloat16)
            return carry

        sweep(bounds[c], bounds[c + 1], mix, 0, MIX_GROUP)
        columns = pl.ds(bounds[c] * LANES, (bounds[c + 1] - bounds[c]) * LANES)
        for k in range(1, groups):
            to = lax.rem(my_dp + k, groups)
            routed.append(pltpu.make_async_remote_copy(
                src_ref=send.at[to, :, columns], dst_ref=landed.at[my_dp, :, columns],
                send_sem=out_ssem.at[c, k], recv_sem=out_rsem.at[c, my_dp],
                device_id=(to, my_v), device_id_type=MESH,
            ))
            routed[-1].start()
        own_copies.append(pltpu.make_async_copy(
            send.at[my_dp, :, columns], landed.at[my_dp, :, columns], local_sem.at[c]))
        own_copies[-1].start()

    sent_accept = zero
    sent_expected = zero
    expected = jnp.broadcast_to(expected, (depth, LANES))
    for n in range(seqs):
        at_slot = lane == slots[n]
        sent_accept = jnp.where(at_slot, accept[:, n:n + 1], sent_accept)
        sent_expected = jnp.where(at_slot, expected[:, n:n + 1], sent_expected)
    for g in range(groups):
        shift = (LANES - g * capacity) % LANES
        small[g, 0:depth, :] = pltpu.roll(sent_accept, shift, 1) if shift else sent_accept
        small[g, depth:2 * depth, :] = pltpu.roll(sent_expected, shift, 1) if shift else sent_expected
    for k in range(1, groups):
        to = lax.rem(my_dp + k, groups)
        routed.append(pltpu.make_async_remote_copy(
            src_ref=small.at[to], dst_ref=small_in.at[my_dp],
            send_sem=sm_ssem.at[k], recv_sem=sm_rsem.at[my_dp],
            device_id=(to, my_v), device_id_type=MESH,
        ))
        routed[-1].start()
    stores = []
    for c in range(CHUNKS):
        columns = pl.ds(bounds[c] * LANES, (bounds[c + 1] - bounds[c]) * LANES)
        for k in range(1, groups):
            source = lax.rem(my_dp + k, groups)
            pltpu.make_async_remote_copy(
                src_ref=send.at[source, :, columns], dst_ref=landed.at[source, :, columns],
                send_sem=out_ssem.at[c, k], recv_sem=out_rsem.at[c, source],
                device_id=(source, my_v), device_id_type=MESH,
            ).wait_recv()
        own_copies[c].wait()

        def gather(base, count, carry):
            span = pl.ds(pl.multiple_of(base * LANES, LANES), count * LANES)
            pieces = [landed[g, :, span].astype(jnp.float32) for g in range(groups)]
            block[:, span] = jnp.concatenate(pieces, axis=0).astype(jnp.bfloat16)
            return carry

        sweep(bounds[c], bounds[c + 1], gather, 0, MIX_GROUP)
        stores.append(pltpu.make_async_copy(block.at[:, columns], out.at[:, columns], store_sem.at[c]))
        stores[-1].start()
    small_in[my_dp] = small[my_dp]
    for k in range(1, groups):
        source = lax.rem(my_dp + k, groups)
        pltpu.make_async_remote_copy(
            src_ref=small.at[source], dst_ref=small_in.at[source],
            send_sem=sm_ssem.at[k], recv_sem=sm_rsem.at[source],
            device_id=(source, my_v), device_id_type=MESH,
        ).wait_recv()
    final_accept = zero
    final_expected = zero
    for g in range(groups):
        mine = (lane >= g * capacity) & (lane < (g + 1) * capacity)
        final_accept = jnp.where(mine, pltpu.roll(small_in[g, 0:depth, :], g * capacity, 1), final_accept)
        final_expected = jnp.where(mine, pltpu.roll(small_in[g, depth:2 * depth, :], g * capacity, 1), final_expected)
    accept_out[...] = final_accept[:, :rows]
    expected_out[...] = final_expected[0:1, :rows]
    for copy in stores:
        copy.wait()
    for copy in stat_copies + spread_copies + routed:
        copy.wait_send()


def body(logits, draft_probs, draft_tokens, draft_lengths, owner_group):
    groups = lax.axis_size("dp")
    vocab = lax.axis_size("vocab")
    seqs, depth, width = logits.shape
    capacity = max(2, 2 * seqs // groups)
    tiles = -(-width // LANES)
    padded = tiles * LANES
    anywhere = pl.BlockSpec(memory_space=pl.ANY)
    hbm = pl.BlockSpec(memory_space=pltpu.HBM)
    dma = pltpu.SemaphoreType.DMA
    slots = groups * capacity
    vmem = pl.BlockSpec(memory_space=pltpu.VMEM)
    out, accept, expected = pl.pallas_call(
        functools.partial(kernel, (groups, vocab, capacity)),
        out_shape=(
            jax.ShapeDtypeStruct((slots, padded), jnp.bfloat16),
            jax.ShapeDtypeStruct((depth, slots), jnp.float32),
            jax.ShapeDtypeStruct((1, slots), jnp.float32),
        ),
        in_specs=[hbm] * 5,
        out_specs=(anywhere, vmem, vmem),
        scratch_shapes=[
            pltpu.SMEM((seqs, depth), jnp.int32),
            pltpu.SMEM((seqs,), jnp.int32),
            pltpu.SMEM((seqs,), jnp.int32),
            pltpu.VMEM((seqs, depth, width), jnp.bfloat16),
            pltpu.VMEM((seqs, depth, width), jnp.bfloat16),
            pltpu.VMEM((tiles, seqs * depth, LANES), jnp.float32),
            pltpu.VMEM((groups, capacity, padded), jnp.bfloat16),
            pltpu.VMEM((groups, capacity, padded), jnp.bfloat16),
            pltpu.VMEM((slots, padded), jnp.bfloat16),
            pltpu.VMEM((vocab, depth, LANES), jnp.float32),
            pltpu.VMEM((vocab, depth, LANES), jnp.float32),
            pltpu.VMEM((groups, 2 * depth, LANES), jnp.float32),
            pltpu.VMEM((groups, 2 * depth, LANES), jnp.float32),
            dma((3,)),
            dma((2 * seqs,)),
            dma((vocab,)),
            dma((vocab,)),
            dma((vocab,)),
            dma((vocab,)),
            dma((CHUNKS, groups)),
            dma((CHUNKS, groups)),
            dma((groups,)),
            dma((groups,)),
            dma((CHUNKS,)),
            dma((CHUNKS,)),
        ],
        compiler_params=pltpu.CompilerParams(
            collective_id=0, has_side_effects=True, vmem_limit_bytes=54500 * 1024
        ),
    )(draft_tokens, draft_lengths, owner_group, logits, draft_probs)
    correction = out[:, :width]
    accept_ratio = accept.T
    expected_accepted = expected.reshape(slots)
    return (correction, accept_ratio, expected_accepted)


def solution(mesh):
    placed = (P("dp", None, "vocab"), P("dp", None, "vocab"), P("dp", None), P("dp"), P("dp"))
    return jax.shard_map(
        body,
        mesh=mesh,
        in_specs=placed,
        out_specs=(P("dp", "vocab"), P("dp", None), P("dp")),
        check_vma=False,
    )
```
